32 devices in a mesh: walker: 8 (over z, core), chol: 4 (over y, x).
Axes of the slice: x: 2, y: 2, z: 4, core: 2. Of those that a mesh axis runs over, the one named last changes fastest.
Arguments:
- chol_vectors: bfloat16 [256, 768, 192], P('chol', 'walker'), may hold values from -0.2 to 0.2, as said below
- green: bfloat16 [16, 768, 192], P('walker'), may hold values from -6 to 6
Outputs:
- energy: float32 [16], P('walker')
- gradient: float32 [16, 768, 192], P('walker', 'chol')
The draws below stay inside these ranges and needn't reach their ends.
Inputs may be any that keep to these rules, and one draw needn't show every extreme that they name: `chol_vectors`: independent entries of each vector; vector magnitudes differ from vector to vector.
All inputs are finite; a program needn't handle non-finite values.
Results may differ from the reference program's by a relative error of at most 0.0042.
Values may be sent and summed in bfloat16 or wider, within the bound.
A program may use at most 128 MiB of HBM per device.

```python
import jax
import jax.numpy as jnp
from jax import lax

M = 768
NOCC = 192
NCHOL = 256
WALKERS = 16


def draw_chol_vectors(key, part):
    index = jnp.arange(NCHOL, dtype=jnp.float32) / (NCHOL - 1)
    decay = 3.0 ** (-0.5 * index)
    values = jax.random.normal(key, (NCHOL, M, NOCC), jnp.float32)
    values = values * M ** (-0.5) * decay[:, None, None]
    return jnp.clip(values, -0.19921875, 0.19921875).astype(jnp.bfloat16)


def block_levels(rng, shape, pieces, least, high):
    def one(dim, shards_of):
        steps = jax.random.uniform(jax.random.fold_in(jax.random.fold_in(rng, 6), dim), (shards_of,), jnp.float32, least / len(pieces), high / len(pieces))
        return jnp.repeat(jnp.exp(steps), shape[dim] // shards_of).reshape((-1,) + (1,) * (len(shape) - dim - 1))

    loudness = one(*pieces[0])
    for cut in pieces[1:]:
        loudness = loudness * one(*cut)
    return loudness


def normal_values(rng, dims, scale, bound, cuts=(), kind=jnp.bfloat16):
    array = jax.random.normal(rng, dims, jnp.float32) * scale
    if len(cuts) > 0:
        array = block_levels(rng, dims, cuts, -0.22, 0.18) * array
    return jnp.clip(array, min=-bound, max=bound).astype(kind)


def setup_inputs(seed: int = 0) -> dict:
    key_list = jax.random.split(jax.random.key(seed), 3)
    chol_vectors = draw_chol_vectors(jax.random.fold_in(key_list[2], 71), 0)
    green = normal_values(key_list[1], (WALKERS, M, NOCC), 1.0, 6.0, ((0, 8),))
    return dict(chol_vectors=chol_vectors, green=green)


def reference(chol_vectors, green):
    factors = chol_vectors.astype(jnp.float32)
    escale = 1.0 / (NCHOL * NOCC)
    gscale = 1.0 / (NCHOL ** 0.5)

    def one_walker(single):
        gfloat = single.astype(jnp.float32)
        tmat = jnp.einsum("kmi,mj->kij", factors, gfloat, precision=lax.Precision.HIGHEST)
        energy = jnp.sum(tmat * jnp.swapaxes(tmat, 1, 2)) * escale
        tround = lax.optimization_barrier(tmat.astype(jnp.bfloat16)).astype(jnp.float32)
        gradient = jnp.einsum("kmi,kji->mj", factors, tround, precision=lax.Precision.HIGHEST) * gscale
        return energy, gradient

    energy, gradient = lax.map(one_walker, green)
    return energy, gradient
```

```python
import functools
import math

import jax
import jax.numpy as jnp
from jax import lax
from jax.experimental import pallas as pl
from jax.experimental.pallas import tpu as pltpu
from jax.sharding import PartitionSpec as P

MESH = pl.DeviceIdType.MESH
CORES = 2
ANY = pl.BlockSpec(memory_space=pl.ANY)


def remote(src, dst, send, recv, device):
    return pltpu.make_async_remote_copy(
        src_ref=src, dst_ref=dst, send_sem=send, recv_sem=recv, device_id=device, device_id_type=MESH
    )


def greet(devices):
    barrier = pltpu.get_barrier_semaphore()
    for device in devices:
        pl.semaphore_signal(barrier, inc=1, device_id=device, device_id_type=MESH)
    pl.semaphore_wait(barrier, len(devices))


def gather_kernel(
    span, groups, chol, green, blocks, greens, own_chol, own_green,
    chol_send, chol_recv, pair_send, pair_recv, green_send, green_recv, share_send, share_recv, local,
):
    walker, group = lax.axis_index("walker"), lax.axis_index("chol")
    chip, core = walker // CORES, walker % CORES
    kept, width = blocks.shape[1], green.shape[1] // groups
    partner = (chip * CORES + 1 - core, group)
    peers = [None] + [lax.rem(chip + d, span) for d in range(1, span)]
    sources = [None] + [lax.rem(chip - d + span, span) for d in range(1, span)]
    sides = [None] + [(walker, lax.rem(group + d, groups)) for d in range(1, groups)]
    greet([partner] + [(z * CORES + core, group) for z in peers[1:]] + sides[1:])

    mine = pl.ds(pl.multiple_of(group * width, math.gcd(width, 16)), width)
    waits = []
    first, quarters = [None], [None]
    for d in range(1, span):
        target = (peers[d] * CORES + core, group)
        quarter = remote(
            green.at[:, mine, :], greens.at[chip, :, mine, :], green_send.at[d], green_recv.at[d], target
        )
        quarter.start()
        quarters.append(quarter)
    for d in range(1, span):
        target = (peers[d] * CORES + core, group)
        block = remote(
            chol.at[pl.ds(peers[d] * kept, kept)], blocks.at[walker], chol_send.at[d], chol_recv.at[d], target
        )
        block.start()
        first.append(block)
    held = chol.at[pl.ds(chip * kept, kept)]
    pair = remote(held, blocks.at[walker], pair_send.at[0], pair_recv.at[0], partner)
    pair.start()
    waits.append(pair)
    takes = [pltpu.make_async_copy(held, own_chol, local.at[0]), pltpu.make_async_copy(green, own_green, local.at[1])]
    for take in takes:
        take.start()
    for take in takes:
        take.wait()
    puts = [
        pltpu.make_async_copy(own_chol, blocks.at[walker], local.at[2]),
        pltpu.make_async_copy(own_green, greens.at[chip], local.at[3]),
    ]
    for put in puts:
        put.start()
    for d in range(1, span):
        quarters[d].wait_recv()
        piece = greens.at[sources[d], :, mine, :]
        for e in range(1, groups):
            share = remote(piece, piece, share_send.at[d, e], share_recv.at[d, e], sides[e])
            share.start()
            waits.append(share)
    for d in range(1, span):
        first[d].wait_recv()
        landed = blocks.at[sources[d] * CORES + core]
        pair = remote(landed, landed, pair_send.at[d], pair_recv.at[d], partner)
        pair.start()
        waits.append(pair)
    for put in puts:
        put.wait()
    for d in range(1, span):
        quarters[d].wait_send()
        first[d].wait_send()
    for copy in waits:
        copy.wait()


def gather(span, groups, chol, green):
    kl, mb, width = chol.shape
    wl, m, _ = green.shape
    kept = kl // span
    dma = pltpu.SemaphoreType.DMA
    return pl.pallas_call(
        functools.partial(gather_kernel, span, groups),
        out_shape=(
            jax.ShapeDtypeStruct((span * CORES, kept, mb, width), chol.dtype),
            jax.ShapeDtypeStruct((span, wl, m, width), green.dtype),
        ),
        in_specs=[ANY, ANY],
        out_specs=(ANY, ANY),
        scratch_shapes=[
            pltpu.VMEM((kept, mb, width), chol.dtype),
            pltpu.VMEM((wl, m, width), green.dtype),
            dma((span,)), dma((span,)), dma((span,)), dma((span,)), dma((span,)), dma((span,)),
            dma((span, groups)), dma((span, groups)), dma((4,)),
        ],
        compiler_params=pltpu.CompilerParams(collective_id=0, has_side_effects=True),
    )(chol, green)


def product_kernel(chol, green, terms, energy, turned, total):
    k = pl.program_id(1)
    walkers = green.shape[0]

    @pl.when(k == 0)
    def _():
        total[...] = jnp.zeros_like(total)
        energy[...] = jnp.zeros_like(energy)

    turned[...] = chol[0].T
    per = math.gcd(walkers, 2)

    def step(n, carry):
        for u in range(per):
            w = n * per + u
            tmat = jnp.dot(turned[...], green[w], preferred_element_type=jnp.float32)
            energy[w] += jnp.sum(tmat * tmat.T, axis=0, keepdims=True)
            total[w] += lax.dot_general(
                chol[0], tmat.astype(jnp.bfloat16), (((1,), (1,)), ((), ())), preferred_element_type=jnp.float32
            )
        return carry

    lax.fori_loop(0, walkers // per, step, 0)

    @pl.when(k == pl.num_programs(1) - 1)
    def _():
        terms[...] = total[...].astype(terms.dtype)


def products(chol, green):
    kept, m, width = chol.shape
    walkers = green.shape[0]
    some = math.gcd(walkers, 8)
    return pl.pallas_call(
        product_kernel,
        out_shape=(
            jax.ShapeDtypeStruct((walkers, m, width), jnp.bfloat16),
            jax.ShapeDtypeStruct((walkers, 1, width), jnp.float32),
        ),
        grid=(walkers // some, kept),
        in_specs=[
            pl.BlockSpec((1, m, width), lambda g, k: (k, 0, 0)),
            pl.BlockSpec((some, m, width), lambda g, k: (g, 0, 0)),
        ],
        out_specs=(
            pl.BlockSpec((some, m, width), lambda g, k: (g, 0, 0)),
            pl.BlockSpec((some, 1, width), lambda g, k: (g, 0, 0)),
        ),
        scratch_shapes=[pltpu.VMEM((width, m), jnp.bfloat16), pltpu.VMEM((some, m, width), jnp.float32)],
        compiler_params=pltpu.CompilerParams(
            dimension_semantics=("arbitrary", "arbitrary"), vmem_limit_bytes=60 * 2**20
        ),
    )(chol, green)


def spread_kernel(span, groups, terms, energy, parts, energies, send, recv, esend, erecv):
    walker, group = lax.axis_index("walker"), lax.axis_index("chol")
    chip, core = walker // CORES, walker % CORES
    wl, width = parts.shape[1], parts.shape[2]
    others = [(d, e) for d in range(span) for e in range(groups) if d + e > 0]
    target = {(d, e): (lax.rem(chip + d, span), lax.rem(group + e, groups)) for d, e in others}
    greet([(target[o][0] * CORES + core, target[o][1]) for o in others])
    copies = []
    for n, o in enumerate(others):
        z, q = target[o]
        device = (z * CORES + core, q)
        block = terms.at[pl.ds(z * wl, wl), pl.ds(pl.multiple_of(q * width, math.gcd(width, 16)), width), :]
        copies.append(remote(block, parts.at[n], send.at[n], recv.at[n], device))
        copies.append(remote(energy.at[z], energies.at[n], esend.at[n], erecv.at[n], device))
    for copy in copies:
        copy.start()
    for copy in copies:
        copy.wait()


def spread(span, groups, terms, energy):
    walkers, m, width = terms.shape
    count = span * groups - 1
    dma = pltpu.SemaphoreType.DMA
    return pl.pallas_call(
        functools.partial(spread_kernel, span, groups),
        out_shape=(
            jax.ShapeDtypeStruct((count, walkers // span, m // groups, width), terms.dtype),
            jax.ShapeDtypeStruct((count,) + energy.shape[1:], energy.dtype),
        ),
        in_specs=[ANY, ANY],
        out_specs=(ANY, ANY),
        scratch_shapes=[dma((count,)), dma((count,)), dma((count,)), dma((count,))],
        compiler_params=pltpu.CompilerParams(collective_id=1, has_side_effects=True),
    )(terms, energy)


def per_device(span, groups, chol_vectors, green):
    kl, mb, width = chol_vectors.shape
    wl, m, _ = green.shape
    nchol = kl * groups
    escale = 1.0 / (nchol * width)
    gscale = 1.0 / nchol**0.5
    chip, group = lax.axis_index("walker") // CORES, lax.axis_index("chol")

    blocks, greens = gather(span, groups, chol_vectors, green)
    chol = jnp.transpose(blocks, (1, 0, 2, 3)).reshape(kl // span, m, width)
    terms, lines = products(chol, greens.reshape(span * wl, m, width))

    sums = jnp.sum(lines, axis=(1, 2)).reshape(span, wl, 1)
    sums = jnp.broadcast_to(sums, (span, wl, 128))
    parts, energies = spread(span, groups, terms, sums)
    own = lax.dynamic_slice(terms, (chip * wl, group * (m // groups), 0), (wl, m // groups, width))
    gradient = (own.astype(jnp.float32) + jnp.sum(parts.astype(jnp.float32), axis=0)) * gscale
    energy = lax.dynamic_index_in_dim(sums, chip, 0, keepdims=False) + jnp.sum(energies, axis=0)
    return energy[:, 0] * escale, gradient


def solution(mesh):
    span, groups = mesh.shape["walker"] // CORES, mesh.shape["chol"]
    return jax.shard_map(
        functools.partial(per_device, span, groups),
        mesh=mesh,
        in_specs=(P("chol", "walker", None), P("walker", None, None)),
        out_specs=(P("walker"), P("walker", "chol", None)),
        check_vma=False,
    )
```

```python
import functools
import math

import jax
import jax.numpy as jnp
from jax import lax
from jax.experimental import pallas as pl
from jax.experimental.pallas import tpu as pltpu
from jax.sharding import PartitionSpec as P

MESH = pl.DeviceIdType.MESH
CORES = 2
ANY = pl.BlockSpec(memory_space=pl.ANY)


def remote(src, dst, send, recv, device):
    return pltpu.make_async_remote_copy(
        src_ref=src, dst_ref=dst, send_sem=send, recv_sem=recv, device_id=device, device_id_type=MESH
    )


def greet(devices):
    barrier = pltpu.get_barrier_semaphore()
    for device in devices:
        pl.semaphore_signal(barrier, inc=1, device_id=device, device_id_type=MESH)
    pl.semaphore_wait(barrier, len(devices))


def gather_kernel(
    span, groups, chol, green, blocks, greens, own_chol, own_green,
    chol_send, chol_recv, pair_send, pair_recv, green_send, green_recv, share_send, share_recv, local,
):
    walker, group = lax.axis_index("walker"), lax.axis_index("chol")
    chip, core = walker // CORES, walker % CORES
    kept, width = blocks.shape[1], green.shape[1] // groups
    partner = (chip * CORES + 1 - core, group)
    peers = [None] + [lax.rem(chip + d, span) for d in range(1, span)]
    sources = [None] + [lax.rem(chip - d + span, span) for d in range(1, span)]
    sides = [None] + [(walker, lax.rem(group + d, groups)) for d in range(1, groups)]
    greet([partner] + [(z * CORES + core, group) for z in peers[1:]] + sides[1:])

    mine = pl.ds(pl.multiple_of(group * width, math.gcd(width, 16)), width)
    waits = []
    first, quarters = [None], [None]
    for d in range(1, span):
        target = (peers[d] * CORES + core, group)
        quarter = remote(
            green.at[:, mine, :], greens.at[chip, :, mine, :], green_send.at[d], green_recv.at[d], target
        )
        quarter.start()
        quarters.append(quarter)
    for d in range(1, span):
        target = (peers[d] * CORES + core, group)
        block = remote(
            chol.at[pl.ds(peers[d] * kept, kept)], blocks.at[walker], chol_send.at[d], chol_recv.at[d], target
        )
        block.start()
        first.append(block)
    held = chol.at[pl.ds(chip * kept, kept)]
    pair = remote(held, blocks.at[walker], pair_send.at[0], pair_recv.at[0], partner)
    pair.start()
    waits.append(pair)
    takes = [pltpu.make_async_copy(held, own_chol, local.at[0]), pltpu.make_async_copy(green, own_green, local.at[1])]
    for take in takes:
        take.start()
    for take in takes:
        take.wait()
    puts = [
        pltpu.make_async_copy(own_chol, blocks.at[walker], local.at[2]),
        pltpu.make_async_copy(own_green, greens.at[chip], local.at[3]),
    ]
    for put in puts:
        put.start()
    for d in range(1, span):
        quarters[d].wait_recv()
        piece = greens.at[sources[d], :, mine, :]
        for e in range(1, groups):
            share = remote(piece, piece, share_send.at[d, e], share_recv.at[d, e], sides[e])
            share.start()
            waits.append(share)
    for d in range(1, span):
        first[d].wait_recv()
        landed = blocks.at[sources[d] * CORES + core]
        pair = remote(landed, landed, pair_send.at[d], pair_recv.at[d], partner)
        pair.start()
        waits.append(pair)
    for put in puts:
        put.wait()
    for d in range(1, span):
        quarters[d].wait_send()
        first[d].wait_send()
    for copy in waits:
        copy.wait()


def gather(span, groups, chol, green):
    kl, mb, width = chol.shape
    wl, m, _ = green.shape
    kept = kl // span
    dma = pltpu.SemaphoreType.DMA
    return pl.pallas_call(
        functools.partial(gather_kernel, span, groups),
        out_shape=(
            jax.ShapeDtypeStruct((span * CORES, kept, mb, width), chol.dtype),
            jax.ShapeDtypeStruct((span, wl, m, width), green.dtype),
        ),
        in_specs=[ANY, ANY],
        out_specs=(ANY, ANY),
        scratch_shapes=[
            pltpu.VMEM((kept, mb, width), chol.dtype),
            pltpu.VMEM((wl, m, width), green.dtype),
            dma((span,)), dma((span,)), dma((span,)), dma((span,)), dma((span,)), dma((span,)),
            dma((span, groups)), dma((span, groups)), dma((4,)),
        ],
        compiler_params=pltpu.CompilerParams(collective_id=0, has_side_effects=True),
    )(chol, green)


def product_kernel(chol, green, terms, energy, turned, total):
    k = pl.program_id(1)
    walkers = green.shape[0]

    @pl.when(k == 0)
    def _():
        total[...] = jnp.zeros_like(total)
        energy[...] = jnp.zeros_like(energy)

    turned[...] = chol[0].T
    per = math.gcd(walkers, 4)

    def step(n, carry):
        for u in range(per):
            w = n * per + u
            tmat = jnp.dot(turned[...], green[w], preferred_element_type=jnp.float32)
            energy[w] += jnp.sum(tmat * tmat.T, axis=0, keepdims=True)
            total[w] += lax.dot_general(
                chol[0], tmat.astype(jnp.bfloat16), (((1,), (1,)), ((), ())), preferred_element_type=jnp.float32
            )
        return carry

    lax.fori_loop(0, walkers // per, step, 0)

    @pl.when(k == pl.num_programs(1) - 1)
    def _():
        terms[...] = total[...].astype(terms.dtype)


def products(chol, green):
    kept, m, width = chol.shape
    walkers = green.shape[0]
    some = math.gcd(walkers, 8)
    return pl.pallas_call(
        product_kernel,
        out_shape=(
            jax.ShapeDtypeStruct((walkers, m, width), jnp.bfloat16),
            jax.ShapeDtypeStruct((walkers, 1, width), jnp.float32),
        ),
        grid=(walkers // some, kept),
        in_specs=[
            pl.BlockSpec((1, m, width), lambda g, k: (k, 0, 0)),
            pl.BlockSpec((some, m, width), lambda g, k: (g, 0, 0)),
        ],
        out_specs=(
            pl.BlockSpec((some, m, width), lambda g, k: (g, 0, 0)),
            pl.BlockSpec((some, 1, width), lambda g, k: (g, 0, 0)),
        ),
        scratch_shapes=[pltpu.VMEM((width, m), jnp.bfloat16), pltpu.VMEM((some, m, width), jnp.float32)],
        compiler_params=pltpu.CompilerParams(
            dimension_semantics=("arbitrary", "arbitrary"), vmem_limit_bytes=60 * 2**20
        ),
    )(chol, green)


def spread_kernel(span, groups, terms, energy, parts, energies, send, recv, esend, erecv):
    walker, group = lax.axis_index("walker"), lax.axis_index("chol")
    chip, core = walker // CORES, walker % CORES
    wl, width = parts.shape[1], parts.shape[2]
    others = [(d, e) for d in range(span) for e in range(groups) if d + e > 0]
    target = {(d, e): (lax.rem(chip + d, span), lax.rem(group + e, groups)) for d, e in others}
    greet([(target[o][0] * CORES + core, target[o][1]) for o in others])
    copies = []
    for n, o in enumerate(others):
        z, q = target[o]
        device = (z * CORES + core, q)
        block = terms.at[pl.ds(z * wl, wl), pl.ds(pl.multiple_of(q * width, math.gcd(width, 16)), width), :]
        copies.append(remote(block, parts.at[n], send.at[n], recv.at[n], device))
        copies.append(remote(energy.at[z], energies.at[n], esend.at[n], erecv.at[n], device))
    for copy in copies:
        copy.start()
    for copy in copies:
        copy.wait()


def spread(span, groups, terms, energy):
    walkers, m, width = terms.shape
    count = span * groups - 1
    dma = pltpu.SemaphoreType.DMA
    return pl.pallas_call(
        functools.partial(spread_kernel, span, groups),
        out_shape=(
            jax.ShapeDtypeStruct((count, walkers // span, m // groups, width), terms.dtype),
            jax.ShapeDtypeStruct((count,) + energy.shape[1:], energy.dtype),
        ),
        in_specs=[ANY, ANY],
        out_specs=(ANY, ANY),
        scratch_shapes=[dma((count,)), dma((count,)), dma((count,)), dma((count,))],
        compiler_params=pltpu.CompilerParams(collective_id=1, has_side_effects=True),
    )(terms, energy)


def per_device(span, groups, chol_vectors, green):
    kl, mb, width = chol_vectors.shape
    wl, m, _ = green.shape
    nchol = kl * groups
    escale = 1.0 / (nchol * width)
    gscale = 1.0 / nchol**0.5
    chip, group = lax.axis_index("walker") // CORES, lax.axis_index("chol")

    blocks, greens = gather(span, groups, chol_vectors, green)
    chol = jnp.transpose(blocks, (1, 0, 2, 3)).reshape(kl // span, m, width)
    terms, lines = products(chol, greens.reshape(span * wl, m, width))

    sums = jnp.sum(lines, axis=(1, 2)).reshape(span, wl, 1)
    sums = jnp.broadcast_to(sums, (span, wl, 128))
    parts, energies = spread(span, groups, terms, sums)
    own = lax.dynamic_slice(terms, (chip * wl, group * (m // groups), 0), (wl, m // groups, width))
    gradient = (own.astype(jnp.float32) + jnp.sum(parts.astype(jnp.float32), axis=0)) * gscale
    energy = lax.dynamic_index_in_dim(sums, chip, 0, keepdims=False) + jnp.sum(energies, axis=0)
    return energy[:, 0] * escale, gradient


def solution(mesh):
    span, groups = mesh.shape["walker"] // CORES, mesh.shape["chol"]
    return jax.shard_map(
        functools.partial(per_device, span, groups),
        mesh=mesh,
        in_specs=(P("chol", "walker", None), P("walker", None, None)),
        out_specs=(P("walker"), P("walker", "chol", None)),
        check_vma=False,
    )
```
